32 devices in a mesh: pair: 4 (over y, x), aux: 8 (over z, core).
Axes of the slice: x: 2, y: 2, z: 4, core: 2. Of those that a mesh axis runs over, the one named last changes fastest.
Arguments:
- same_panels: bfloat16 [32, 2, 112, 59904], P('aux', None, None, 'pair'), may hold values from -1 to 1
- opposite_panels: bfloat16 [32, 2, 112, 59904], P('aux', None, None, 'pair'), may hold values from -1 to 1
- same_amplitudes: bfloat16 [32, 112, 112], replicated, may hold values from -2 to 2
- opposite_amplitudes: bfloat16 [32, 112, 112], replicated, may hold values from -2 to 2
- same_energies: float32 [32, 2, 112], replicated, may hold values from 0.5 to 3
- opposite_energies: float32 [32, 2, 112], replicated, may hold values from 0.5 to 3
- same_ranks: int32 [32], replicated, may hold values from 48 to 112
- opposite_ranks: int32 [32], replicated, may hold values from 48 to 112
Outputs:
- same_residual: float32 [32, 112, 112], P('pair', 'aux')
- opposite_residual: float32 [32, 112, 112], P('pair', 'aux')
The draws below stay inside these ranges and needn't reach their ends.
Inputs may be any that keep to these rules, and one draw needn't show every extreme that they name: `same_ranks`: slots at or beyond a pair's rank are padding. `opposite_ranks`: slots at or beyond a pair's rank are padding.
All inputs are finite; a program needn't handle non-finite values.
Results may differ from the reference program's by a relative error of at most 0.0013.
Values may be sent and summed in bfloat16 or wider, within the bound.
A program may use at most 128 MiB of HBM per device.

```python
import math
import jax
import jax.numpy as jnp
from jax import lax

R = 112
NAUX = 59904
PAIRS = 32


def with_ends(entries, key, least, top_value):
    dims = entries.shape
    index_at = [jax.random.randint(jax.random.fold_in(key, axis), (), 0, dims[axis]) for axis in range(len(dims))]
    entries = entries.at[tuple(index_at)].set(least)
    longest = dims.index(max(dims))
    index_at[longest] = (index_at[longest] + 1) % dims[longest]
    return entries.at[tuple(index_at)].set(top_value)


def steps_of(own_key, extent, shards, smallest, largest):
    def one(position, parts):
        heights = jax.random.uniform(jax.random.fold_in(jax.random.fold_in(own_key, 6), position), (parts,), jnp.float32, smallest / len(shards), largest / len(shards))
        return jnp.repeat(jnp.exp(heights), extent[position] // parts).reshape((-1,) + (1,) * (len(extent) - position - 1))

    level = one(*shards[0])
    for cut in shards[1:]:
        level = level * one(*cut)
    return level


def bell_draw(stream_key, shape, deviation, limit, pieces=(), kind=jnp.bfloat16):
    factor_of = steps_of(stream_key, shape, pieces, -0.22, 0.18) if pieces else 1.0
    values = jax.random.normal(stream_key, shape, jnp.float32) * deviation * factor_of
    return jnp.minimum(jnp.maximum(values, -limit), limit).astype(kind)


def setup_inputs(seed: int = 0) -> dict:
    arg_keys = jax.random.split(jax.random.key(seed), 9)
    same_panels = bell_draw(arg_keys[0], (PAIRS, 2, R, NAUX), (NAUX ** -0.25), 1.0, ((0, 8), (3, 4)))
    opposite_panels = bell_draw(arg_keys[1], (PAIRS, 2, R, NAUX), (NAUX ** -0.25), 1.0, ((0, 8), (3, 4)))
    same_amplitudes = bell_draw(arg_keys[2], (PAIRS, R, R), 0.15, 2.0)
    opposite_amplitudes = bell_draw(arg_keys[3], (PAIRS, R, R), 0.15, 2.0)
    same_energies = jnp.clip(jnp.exp(jax.random.uniform(arg_keys[4], (PAIRS, 2, R), jnp.float32, math.log(0.5), math.log(3.0))), 0.5, 3.0)
    opposite_energies = jnp.clip(jnp.exp(jax.random.uniform(arg_keys[5], (PAIRS, 2, R), jnp.float32, math.log(0.5), math.log(3.0))), 0.5, 3.0)
    same_ranks = with_ends(jax.random.randint(arg_keys[6], (PAIRS,), R * 3 // 7, R + 1), jax.random.fold_in(arg_keys[6], 1), R * 3 // 7, R).astype(jnp.int32)
    opposite_ranks = with_ends(jax.random.randint(arg_keys[7], (PAIRS,), R * 3 // 7, R + 1), jax.random.fold_in(arg_keys[7], 1), R * 3 // 7, R).astype(jnp.int32)
    return dict(same_panels=same_panels, opposite_panels=opposite_panels, same_amplitudes=same_amplitudes, opposite_amplitudes=opposite_amplitudes, same_energies=same_energies, opposite_energies=opposite_energies, same_ranks=same_ranks, opposite_ranks=opposite_ranks)


def slot_mask(ranks):
    slots = jnp.arange(R, dtype=jnp.int32)
    return (slots[None, :] < ranks[:, None]).astype(jnp.float32)


def masked_amplitudes(amplitudes, keep):
    outer = keep[:, :, None] * keep[:, None, :]
    return (amplitudes.astype(jnp.float32) * outer).astype(jnp.bfloat16)


def dressing_rows(panels, masked):
    def one_pair(items):
        panel, amplitude = items
        mixed = jnp.dot(amplitude, panel[1], preferred_element_type=jnp.float32)
        return jnp.sum(panel[0].astype(jnp.float32) * mixed, axis=0)
    return lax.map(one_pair, (panels, masked))


def residual_rows(panels, masked, energies, keep, coupling):
    def one_pair(items):
        panel, amplitude, energy, mask_row = items
        exchange = jnp.dot(panel[0], panel[1].T, preferred_element_type=jnp.float32)
        scaled = (panel[0].astype(jnp.float32) * coupling[None, :]).astype(jnp.bfloat16)
        coulomb = jnp.dot(scaled, panel[1].T, preferred_element_type=jnp.float32)
        diagonal = (energy[0][:, None] + energy[1][None, :]) * amplitude.astype(jnp.float32)
        return (exchange + coulomb + diagonal) * (mask_row[:, None] * mask_row[None, :])
    return lax.map(one_pair, (panels, masked, energies, keep))


def reference(same_panels, opposite_panels, same_amplitudes, opposite_amplitudes, same_energies, opposite_energies, same_ranks, opposite_ranks):
    same_keep = slot_mask(same_ranks)
    opposite_keep = slot_mask(opposite_ranks)
    same_masked = masked_amplitudes(same_amplitudes, same_keep)
    opposite_masked = masked_amplitudes(opposite_amplitudes, opposite_keep)
    coupling = jnp.sum(dressing_rows(same_panels, same_masked), axis=0) + jnp.sum(dressing_rows(opposite_panels, opposite_masked), axis=0)
    same_residual = residual_rows(same_panels, same_masked, same_energies, same_keep, coupling)
    opposite_residual = residual_rows(opposite_panels, opposite_masked, opposite_energies, opposite_keep, coupling)
    return same_residual, opposite_residual
```

```python
import functools

import jax
import jax.numpy as jnp
from jax import lax
from jax.experimental import pallas as pl
from jax.experimental.pallas import tpu as pltpu
from jax.sharding import PartitionSpec as P

LANES = 128
GROUP = 2


def slot_mask(ranks, slots):
    places = jnp.arange(slots, dtype=jnp.int32)
    return (places[None, :] < ranks[:, None]).astype(jnp.float32)


def masked_amplitudes(amplitudes, keep):
    outer = keep[:, :, None] * keep[:, None, :]
    return (amplitudes.astype(jnp.float32) * outer).astype(jnp.bfloat16)


def finish_rows(summed, amplitudes, energies, ranks, pair_start, row_start):
    count = summed.shape[0]
    rows = summed.shape[1]
    slots = amplitudes.shape[1]
    keep = slot_mask(lax.dynamic_slice_in_dim(ranks, pair_start, count, 0), slots)
    amplitude = lax.dynamic_slice_in_dim(amplitudes, pair_start, count, 0)
    masked = masked_amplitudes(amplitude, keep)
    masked_rows = lax.dynamic_slice_in_dim(masked, row_start, rows, 1).astype(jnp.float32)
    energy = lax.dynamic_slice_in_dim(energies, pair_start, count, 0)
    first_gap = lax.dynamic_slice_in_dim(energy[:, 0], row_start, rows, 1)
    keep_rows = lax.dynamic_slice_in_dim(keep, row_start, rows, 1)
    diagonal = (first_gap[:, :, None] + energy[:, 1][:, None, :]) * masked_rows
    return (summed + diagonal) * (keep_rows[:, :, None] * keep[:, None, :])


def local_masked(amplitudes, ranks, start, count):
    slots = amplitudes.shape[1]
    keep = slot_mask(lax.dynamic_slice_in_dim(ranks, start, count, 0), slots)
    return masked_amplitudes(lax.dynamic_slice_in_dim(amplitudes, start, count, 0), keep)


def rows_dot(first, second):
    return lax.dot_general(
        first, second, (((1,), (1,)), ((), ())), preferred_element_type=jnp.float32
    )


def kernel(
    plan,
    same_ref,
    opposite_ref,
    masked_ref,
    same_out,
    opposite_out,
    panel,
    total,
    partial,
    flat,
    share,
    arrived,
    gathered,
    out_a,
    in_a,
    out_b,
    in_b,
    load_sem,
    scatter_send,
    scatter_recv,
    gather_send,
    gather_recv,
    a_send,
    a_recv,
    b_send,
    b_recv,
):
    pairs, auxes, count, slots, steps, width, chunk = plan
    sources = (same_ref, opposite_ref)
    fold = auxes // pairs
    rows = slots // auxes
    block = 2 * count
    groups = block // GROUP
    me_pair = lax.axis_index("pair")
    me_aux = lax.axis_index("aux")

    def load(step, spin, pair):
        at = pl.ds(pl.multiple_of(step * width, LANES), width)
        return pltpu.make_async_copy(
            sources[spin].at[pair, :, :, at],
            panel.at[spin * count + pair, :, :, at],
            load_sem.at[step, spin * count + pair],
        )

    @pl.loop(0, steps)
    def _(step):
        @pl.loop(0, count)
        def _(pair):
            load(step, 0, pair).start()
            load(step, 1, pair).start()

    barrier = pltpu.get_barrier_semaphore()
    devices = pairs * auxes
    me = me_pair * auxes + me_aux

    @pl.loop(1, devices)
    def _(ahead):
        other = lax.rem(me + ahead, devices)
        pl.semaphore_signal(
            barrier,
            inc=1,
            device_id=(lax.div(other, auxes), lax.rem(other, auxes)),
            device_id_type=pl.DeviceIdType.MESH,
        )

    total[...] = jnp.zeros_like(total)
    flat[...] = jnp.zeros_like(flat)

    def lanes(step):
        return pl.ds(pl.multiple_of(step * width, LANES), width)

    def exchange(place, step):
        at = lanes(step)
        total[place] += rows_dot(panel[place, 0, :, at], panel[place, 1, :, at])

    def dress(place, step):
        at = lanes(step)
        mixed = jnp.dot(
            masked_ref[place], panel[place, 1, :, at], preferred_element_type=jnp.float32
        )
        product = panel[place, 0, :, at].astype(jnp.float32) * mixed
        return jnp.sum(product.reshape(slots // 8, 8, width), axis=0)

    @pl.loop(0, steps)
    def _(step):
        partial[...] = jnp.zeros_like(partial)

        @pl.loop(0, count - 1)
        def _(pair):
            load(step, 0, pair).wait()
            load(step, 1, pair).wait()
            partial[...] += dress(pair, step) + dress(count + pair, step)
            exchange(pair, step)
            exchange(count + pair, step)

        load(step, 0, count - 1).wait()
        load(step, 1, count - 1).wait()
        summed = partial[...] + dress(count - 1, step) + dress(block - 1, step)
        flat[:, lanes(step)] = jnp.sum(summed, axis=0, keepdims=True)

    for part in range(auxes):
        share[part] = flat[:, part * chunk : (part + 1) * chunk]

    pl.semaphore_wait(barrier, devices - 1)

    def peer_aux(ahead):
        return lax.rem(me_aux + ahead, auxes)

    def scatter(ahead):
        other = peer_aux(ahead)
        return pltpu.make_async_remote_copy(
            src_ref=share.at[other],
            dst_ref=arrived.at[ahead],
            send_sem=scatter_send.at[ahead],
            recv_sem=scatter_recv.at[ahead],
            device_id=(me_pair, other),
            device_id_type=pl.DeviceIdType.MESH,
        )

    def gather(ahead):
        return pltpu.make_async_remote_copy(
            src_ref=gathered.at[me_aux],
            dst_ref=gathered.at[me_aux],
            send_sem=gather_send.at[ahead],
            recv_sem=gather_recv.at[ahead],
            device_id=(me_pair, peer_aux(ahead)),
            device_id_type=pl.DeviceIdType.MESH,
        )

    def gather_arrival(ahead):
        source = lax.rem(me_aux + auxes - ahead, auxes)
        return pltpu.make_async_remote_copy(
            src_ref=gathered.at[source],
            dst_ref=gathered.at[source],
            send_sem=gather_send.at[ahead],
            recv_sem=gather_recv.at[ahead],
            device_id=(me_pair, source),
            device_id_type=pl.DeviceIdType.MESH,
        )

    for ahead in range(1, auxes):
        scatter(ahead).start()

    @pl.loop(0, steps)
    def _(step):
        exchange(count - 1, step)

    mine = share[me_aux]
    for ahead in range(1, auxes):
        scatter(ahead).wait_recv()
        mine = mine + arrived[ahead]
    gathered[me_aux] = mine
    for ahead in range(1, auxes):
        gather(ahead).start()

    @pl.loop(0, steps)
    def _(step):
        exchange(block - 1, step)

    for ahead in range(1, auxes):
        gather_arrival(ahead).wait_recv()
    for part in range(auxes):
        flat[:, part * chunk : (part + 1) * chunk] = gathered[part]

    def send_a(group, ahead):
        other = lax.rem(me_pair + ahead, pairs)
        return pltpu.make_async_remote_copy(
            src_ref=out_a.at[other, group],
            dst_ref=in_a.at[ahead, group],
            send_sem=a_send.at[ahead, group],
            recv_sem=a_recv.at[ahead, group],
            device_id=(other, me_aux),
            device_id_type=pl.DeviceIdType.MESH,
        )

    owner = lax.div(me_aux, fold)
    slot = lax.rem(me_aux, fold)

    def send_b(group, part):
        return pltpu.make_async_remote_copy(
            src_ref=out_b.at[group, part],
            dst_ref=in_b.at[slot, group],
            send_sem=b_send.at[part, group],
            recv_sem=b_recv.at[slot, group],
            device_id=(owner, me_pair * fold + part),
            device_id_type=pl.DeviceIdType.MESH,
        )

    def stays(part):
        return jnp.logical_and(owner == me_pair, me_pair * fold + part == me_aux)

    def from_here(part):
        return jnp.logical_and(
            lax.div(me_aux, fold) == me_pair, me_pair * fold + part == me_aux
        )

    def arrival_b(group, part):
        return pltpu.make_async_remote_copy(
            src_ref=out_b.at[group, part],
            dst_ref=in_b.at[part, group],
            send_sem=b_send.at[part, group],
            recv_sem=b_recv.at[part, group],
            device_id=(owner, me_pair * fold + part),
            device_id_type=pl.DeviceIdType.MESH,
        )

    def forward(group):
        held = out_a[me_pair, group]
        for ahead in range(1, pairs):
            send_a(group, ahead).wait_recv()
            held = held + in_a[ahead, group]
        out_b[group] = held
        for part in range(fold):

            @pl.when(jnp.logical_not(stays(part)))
            def _():
                send_b(group, part).start()

            @pl.when(stays(part))
            def _():
                in_b[part, group] = out_b[group, part]

    for group in range(groups):
        for inner in range(GROUP):
            place = group * GROUP + inner

            @pl.loop(0, steps)
            def _(step):
                at = lanes(step)
                scaled = (panel[place, 0, :, at].astype(jnp.float32) * flat[:, at]).astype(
                    jnp.bfloat16
                )
                total[place] += rows_dot(scaled, panel[place, 1, :, at])

            value = total[place]
            for quarter in range(pairs):
                for part in range(fold):
                    first = (quarter * fold + part) * rows
                    out_a[quarter, group, part, inner, 0:rows, 0:slots] = value[
                        first : first + rows, :
                    ]
        for ahead in range(1, pairs):
            send_a(group, ahead).start()
        if group > 0:
            forward(group - 1)
    forward(groups - 1)

    outs = (same_out, opposite_out)
    for group in range(groups):
        for part in range(fold):

            @pl.when(jnp.logical_not(from_here(part)))
            def _():
                arrival_b(group, part).wait_recv()

            for inner in range(GROUP):
                place = group * GROUP + inner
                outs[place // count][part * count + place % count] = in_b[part, group, inner]

    for ahead in range(1, auxes):
        scatter(ahead).wait_send()
        gather(ahead).wait_send()
    for group in range(groups):
        for ahead in range(1, pairs):
            send_a(group, ahead).wait_send()
        for part in range(fold):

            @pl.when(jnp.logical_not(stays(part)))
            def _():
                send_b(group, part).wait_send()


def residual_sums(same_panels, opposite_panels, masked, pairs, auxes):
    if same_panels.shape[3] % LANES:
        extra = ((0, 0), (0, 0), (0, 0), (0, -same_panels.shape[3] % (8 * LANES)))
        same_panels = jnp.pad(same_panels, extra)
        opposite_panels = jnp.pad(opposite_panels, extra)
    count, _, slots, length = same_panels.shape
    tiles = length // LANES
    steps = next(parts for parts in range(min(8, tiles), tiles + 1) if tiles % parts == 0)
    width = length // steps
    chunk = -(-tiles // (8 * auxes)) * 8 * LANES
    fold = auxes // pairs
    rows = slots // auxes
    tall = -(-rows // 8) * 8
    wide = -(-slots // LANES) * LANES
    block = 2 * count
    groups = block // GROUP
    plan = (pairs, auxes, count, slots, steps, width, chunk)
    piece = (GROUP, tall, wide)
    shape = jax.ShapeDtypeStruct((count * fold, tall, wide), jnp.float32)
    anywhere = pl.BlockSpec(memory_space=pl.ANY)
    vmem = pl.BlockSpec(memory_space=pltpu.VMEM)
    dma = pltpu.SemaphoreType.DMA
    return pl.pallas_call(
        functools.partial(kernel, plan),
        out_shape=(shape, shape),
        in_specs=[anywhere, anywhere, vmem],
        out_specs=(vmem, vmem),
        scratch_shapes=[
            pltpu.VMEM((block, 2, slots, length), jnp.bfloat16),
            pltpu.VMEM((block, slots, slots), jnp.float32),
            pltpu.VMEM((8, width), jnp.float32),
            pltpu.VMEM((1, auxes * chunk + 8 * LANES), jnp.float32),
            pltpu.VMEM((auxes, 1, chunk), jnp.float32),
            pltpu.VMEM((auxes, 1, chunk), jnp.float32),
            pltpu.VMEM((auxes, 1, chunk), jnp.float32),
            pltpu.VMEM((pairs, groups, fold) + piece, jnp.float32),
            pltpu.VMEM((pairs, groups, fold) + piece, jnp.float32),
            pltpu.VMEM((groups, fold) + piece, jnp.float32),
            pltpu.VMEM((fold, groups) + piece, jnp.float32),
            dma((steps, block)),
            dma((auxes,)),
            dma((auxes,)),
            dma((auxes,)),
            dma((auxes,)),
            dma((pairs, groups)),
            dma((pairs, groups)),
            dma((fold, groups)),
            dma((fold, groups)),
        ],
        compiler_params=pltpu.CompilerParams(
            collective_id=0, has_side_effects=True, vmem_limit_bytes=67043328
        ),
        name="residual_sums",
    )(same_panels, opposite_panels, masked)


def body(
    pairs,
    auxes,
    same_panels,
    opposite_panels,
    same_amplitudes,
    opposite_amplitudes,
    same_energies,
    opposite_energies,
    same_ranks,
    opposite_ranks,
):
    count = same_panels.shape[0]
    pair_index = lax.axis_index("pair")
    aux_index = lax.axis_index("aux")
    owned = count * auxes // pairs
    rows = same_amplitudes.shape[1] // auxes
    start = aux_index * count
    masked = jnp.concatenate(
        [
            local_masked(same_amplitudes, same_ranks, start, count),
            local_masked(opposite_amplitudes, opposite_ranks, start, count),
        ]
    )
    same_sum, opposite_sum = residual_sums(same_panels, opposite_panels, masked, pairs, auxes)
    same_sum = same_sum[:, :rows, : same_amplitudes.shape[1]]
    opposite_sum = opposite_sum[:, :rows, : same_amplitudes.shape[1]]
    pair_start = pair_index * owned
    row_start = aux_index * rows
    same_residual = finish_rows(
        same_sum, same_amplitudes, same_energies, same_ranks, pair_start, row_start
    )
    opposite_residual = finish_rows(
        opposite_sum, opposite_amplitudes, opposite_energies, opposite_ranks, pair_start, row_start
    )
    return (same_residual, opposite_residual)


def solution(mesh):
    placed = (P("aux", None, None, "pair"),) * 2 + (P(),) * 6
    return jax.shard_map(
        functools.partial(body, mesh.shape["pair"], mesh.shape["aux"]),
        mesh=mesh,
        in_specs=placed,
        out_specs=(P("pair", "aux", None), P("pair", "aux", None)),
        check_vma=False,
    )
```
